256 devices in a mesh: blk: 64 (over x, y_hi, z), rep: 4 (over y_lo, core).
Axes of the slice: x: 4, y: 4 (y_hi: 2, y_lo: 2; y = y_hi * 2 + y_lo), z: 8, core: 2. Of those that a mesh axis runs over, the one named last changes fastest.
Arguments:
- embeddings: float32 [131072, 768], P(('blk', 'rep')), may hold values from -6 to 6
- ranks: int32 [131072], replicated, may hold values from 0 to 131071, each once
Outputs:
- earlier_best: float32 [131072], P(('blk', 'rep'))
- later_best: float32 [131072], P(('blk', 'rep'))
The draws below stay inside these ranges and needn't reach their ends.
Inputs may be any that keep to these rules, and one draw needn't show every extreme that they name: ranks is a permutation of 0 .. 131071.
All inputs are finite; a program needn't handle non-finite values.
Results may differ from the reference program's by a relative error of at most 0.0012.
Values may be sent and summed in bfloat16 or wider, within the bound.
No kernel may reach another device: no remote copies, remote signals or barrier semaphores. Data moves between devices by JAX's collectives and lax.ppermute only.
A program may use at most 64 MiB of HBM per device.

```python
import jax
import jax.numpy as jnp
from jax import lax

D = 768
STEPS = 3
BLOCK = 2048
N = 131072
N_BLK = 64


def levels(rng, shape, cuts, low, top_value):
    def one(position, blocks):
        steps = jax.random.uniform(jax.random.fold_in(jax.random.fold_in(rng, 6), position), (blocks,), jnp.float32, low / len(cuts), top_value / len(cuts))
        return jnp.repeat(jnp.exp(steps), shape[position] // blocks).reshape((-1,) + (1,) * (len(shape) - position - 1))

    level = one(*cuts[0])
    for cut in cuts[1:]:
        level = level * one(*cut)
    return level


def noise(own_key, shape, spread, reach, shards=(), held_as=jnp.bfloat16):
    array = spread * jax.random.normal(own_key, shape, jnp.float32)
    if shards:
        array = array * levels(own_key, shape, shards, -0.22, 0.18)
    return jnp.clip(array, -reach, reach).astype(held_as)


def setup_inputs(seed: int = 0) -> dict:
    arg_keys = jax.random.split(jax.random.key(seed), 3)
    embeddings = noise(arg_keys[0], (N, D), 1.0, 6.0, ((0, 256),), jnp.float32)
    ranks = jax.random.permutation(arg_keys[1], N).astype(jnp.int32)
    return dict(embeddings=embeddings, ranks=ranks)


def reference(embeddings, ranks):
    squares = lax.optimization_barrier(jnp.sum(embeddings * embeddings, axis=1, keepdims=True))
    unit = (embeddings * lax.rsqrt(squares + 1e-06)).astype(jnp.bfloat16).astype(jnp.float32)
    units = unit.reshape(N_BLK, BLOCK, D)
    ordered = ranks.reshape(N_BLK, BLOCK)

    def one_block(index):
        host = units[index]
        host_rank = ordered[index]
        row_best = jnp.full((BLOCK,), -1.0, jnp.float32)
        columns = []
        for offset in range(STEPS + 1):
            other = (index - offset) % N_BLK
            scores = jnp.dot(host, units[other].T, precision=lax.Precision.HIGHEST, preferred_element_type=jnp.float32)
            kept = jnp.where(ordered[other][None, :] < host_rank[:, None], scores, jnp.float32(-1.0))
            row_best = jnp.maximum(row_best, lax.optimization_barrier(jnp.max(kept, axis=1)))
            columns.append(lax.optimization_barrier(jnp.max(kept, axis=0)))
        return (row_best, jnp.stack(columns))
    row_best, column_best = lax.map(one_block, jnp.arange(N_BLK, dtype=jnp.int32))
    later = column_best[:, 0]
    for offset in range(1, STEPS + 1):
        later = jnp.maximum(later, jnp.roll(column_best[:, offset], -offset, axis=0))
    return (row_best.reshape(N), later.reshape(N))
```

```python
import jax
import jax.numpy as jnp
from jax import lax
from jax.sharding import PartitionSpec as P


AXES = ("blk", "rep")
LINE = 8
LOW = -1.0


def routes(blocks, move):
    pairs = []
    for block in range(blocks):
        for place in range(4):
            to_block, to_place = move(block, place)
            pairs.append((4 * block + place, to_block % blocks * 4 + to_place))
    return pairs


def onward(block, place):
    return block + 1, place ^ 2 if block % LINE == LINE - 1 else place


def onward_twice(block, place):
    return onward(*onward(block, place))


def back(block, place):
    return block - 1, place ^ 2 if block % LINE == 0 else place


def back_twice(block, place):
    return back(*back(block, place))


def other(bits):
    return lambda block, place: (block, place ^ bits)


def scores_of(left, right):
    return lax.dot_general(
        left, right, (((1,), (1,)), ((), ())), preferred_element_type=jnp.float32
    )


def best_pair(host, host_rank, visit, visit_rank):
    kept = jnp.where(
        visit_rank[None, :] < host_rank[:, None], scores_of(host, visit), jnp.float32(LOW)
    )
    return jnp.max(kept, axis=1), jnp.max(kept, axis=0)


def both_ways(own, own_rank, peer, peer_rank):
    scores = scores_of(own, peer)
    earlier = jnp.where(peer_rank[None, :] < own_rank[:, None], scores, jnp.float32(LOW))
    later = jnp.where(own_rank[:, None] < peer_rank[None, :], scores, jnp.float32(LOW))
    return jnp.max(earlier, axis=1), jnp.max(later, axis=1)


def largest(values):
    best = values[0]
    for value in values[1:]:
        best = jnp.maximum(best, value)
    return best


def shards(embeddings, ranks):
    rows = embeddings.shape[0]
    blocks = lax.axis_size("blk")
    block = lax.axis_index("blk")
    place = lax.axis_index("rep")

    def send(value, move):
        return lax.ppermute(value, AXES, routes(blocks, move))

    def ranks_of(block_id, place_id):
        start = (block_id * 4 + place_id) * rows
        return lax.dynamic_slice_in_dim(ranks, start, rows)

    squares = jnp.sum(embeddings * embeddings, axis=1, keepdims=True)
    unit = (embeddings * lax.rsqrt(squares + 1e-06)).astype(jnp.bfloat16)

    across = send(unit, other(2))
    beside = send(unit, other(1))
    visit1 = send(unit, onward)
    ahead = send(unit, back)
    across_beside = send(across, other(1))
    visit2 = send(visit1, onward)
    ahead_across = send(ahead, other(2))
    ahead_beside = send(ahead, other(1))
    ahead_both = send(ahead_across, other(1))

    host = [unit, beside, across, across_beside]
    host_ranks = [ranks_of(block, place ^ k) for k in range(4)]
    prev = (block + blocks - 1) % blocks
    prev2 = (block + blocks - 2) % blocks
    nxt = (block + 1) % blocks
    prev_place = jnp.where(block % LINE == 0, place ^ 2, place)
    prev2_place = jnp.where(block % LINE <= 1, place ^ 2, place)
    next_place = jnp.where(nxt % LINE == 0, place ^ 2, place)
    rank1 = ranks_of(prev, prev_place)
    rank2 = ranks_of(prev2, prev2_place)
    front = [ahead, ahead_beside, ahead_across, ahead_both]
    front_ranks = [ranks_of(nxt, next_place ^ k) for k in range(4)]

    own = [both_ways(unit, host_ranks[0], peer, rank) for peer, rank in zip(host, host_ranks)]
    earlier = largest([pair[0] for pair in own])
    later = largest([pair[1] for pair in own])

    one = [best_pair(peer, rank, visit1, rank1) for peer, rank in zip(host, host_ranks)]
    later = jnp.maximum(later, send(largest([pair[1] for pair in one]), back))

    two = [best_pair(peer, rank, visit2, rank2) for peer, rank in zip(host, host_ranks)]
    three = [best_pair(peer, rank, visit2, rank2) for peer, rank in zip(front, front_ranks)]
    columns = largest([pair[1] for pair in two + three])
    later = jnp.maximum(later, send(columns, back_twice))

    front_rows = send(jnp.stack([pair[0] for pair in three]), onward)
    host_rows = jnp.stack([jnp.maximum(a[0], b[0]) for a, b in zip(one, two)])
    merged = jnp.maximum(host_rows, front_rows)
    earlier = jnp.maximum(earlier, merged[0])
    for k in range(1, 4):
        earlier = jnp.maximum(earlier, send(merged[k], other(k)))
    return earlier, later


def solution(mesh):
    return jax.shard_map(
        shards,
        mesh=mesh,
        in_specs=(P(("blk", "rep"), None), P()),
        out_specs=(P(("blk", "rep")), P(("blk", "rep"))),
        check_vma=False,
    )
```

```python
import jax
import jax.numpy as jnp
from jax import lax
from jax.sharding import PartitionSpec as P


AXES = ("blk", "rep")
LINE = 8
LOW = -1.0


def routes(blocks, move):
    pairs = []
    for block in range(blocks):
        for place in range(4):
            target = move(block, place)
            if target is not None:
                pairs.append((4 * block + place, target[0] % blocks * 4 + target[1]))
    return pairs


def onward(block, place):
    return block + 1, place ^ 2 if block % LINE == LINE - 1 else place


def back(block, place):
    return block - 1, place ^ 2 if block % LINE == 0 else place


def back_twice(block, place):
    return back(*back(block, place))


def other(bits):
    return lambda block, place: (block, place ^ bits)


def scores_of(left, right):
    return lax.dot_general(
        left, right, (((1,), (1,)), ((), ())), preferred_element_type=jnp.float32
    )


def best_pair(host, host_rank, visit, visit_rank):
    kept = jnp.where(
        visit_rank[None, :] < host_rank[:, None], scores_of(host, visit), jnp.float32(LOW)
    )
    return jnp.max(kept, axis=1), jnp.max(kept, axis=0)


def both_ways(own, own_rank, peer, peer_rank):
    scores = scores_of(own, peer)
    earlier = jnp.where(peer_rank[None, :] < own_rank[:, None], scores, jnp.float32(LOW))
    later = jnp.where(own_rank[:, None] < peer_rank[None, :], scores, jnp.float32(LOW))
    return jnp.max(earlier, axis=1), jnp.max(later, axis=1)


def largest(values):
    best = values[0]
    for value in values[1:]:
        best = jnp.maximum(best, value)
    return best


def shards(embeddings, ranks):
    rows = embeddings.shape[0]
    blocks = lax.axis_size("blk")
    block = lax.axis_index("blk")
    place = lax.axis_index("rep")
    z = block % LINE

    def send(value, move):
        return lax.ppermute(value, AXES, routes(blocks, move))

    def ranks_of(block_id, place_id):
        start = (block_id * 4 + place_id) * rows
        return lax.dynamic_slice_in_dim(ranks, start, rows)

    squares = jnp.sum(embeddings * embeddings, axis=1, keepdims=True)
    unit = (embeddings * lax.rsqrt(squares + 1e-06)).astype(jnp.bfloat16)

    visit1 = send(unit, onward)
    ahead = send(unit, back)
    across = send(unit, other(2))
    beside = send(unit, other(1))
    visit2 = send(visit1, onward)
    ahead_across = send(ahead, other(2))
    across_beside = send(across, other(1))
    ahead_beside = send(ahead, other(1))
    ahead_both = send(ahead_across, other(1))

    host = [unit, beside, across, across_beside]
    host_ranks = [ranks_of(block, place ^ k) for k in range(4)]
    prev = (block + blocks - 1) % blocks
    prev2 = (block + blocks - 2) % blocks
    nxt = (block + 1) % blocks
    prev_place = jnp.where(z == 0, place ^ 2, place)
    prev2_place = jnp.where(z <= 1, place ^ 2, place)
    next_place = jnp.where(z == LINE - 1, place ^ 2, place)
    rank1 = ranks_of(prev, prev_place)
    rank2 = ranks_of(prev2, prev2_place)
    front = [ahead, ahead_beside, ahead_across, ahead_both]
    front_ranks = [ranks_of(nxt, next_place ^ k) for k in range(4)]

    def tiles(pair, left, left_ranks, right, right_rank):
        out = []
        for k in range(4):
            out.append(pair(left[k], left_ranks[k], right, right_rank))
        return out

    own = []
    for k in range(4):
        own.append(both_ways(unit, host_ranks[0], host[k], host_ranks[k]))
    earlier = largest([pair[0] for pair in own])
    later = largest([pair[1] for pair in own])

    one = tiles(best_pair, host, host_ranks, visit1, rank1)
    two = tiles(best_pair, front, front_ranks, visit1, rank1)
    columns1 = largest([pair[1] for pair in one + two])
    three = tiles(best_pair, front, front_ranks, visit2, rank2)
    columns2 = largest([pair[1] for pair in three])
    front_rows = jnp.stack([jnp.maximum(a[0], b[0]) for a, b in zip(two, three)])
    host_rows = jnp.stack([pair[0] for pair in one])

    merged = jnp.maximum(host_rows, send(front_rows, onward))
    later = jnp.maximum(later, send(columns1, back))
    later = jnp.maximum(later, send(columns2, back_twice))
    earlier = jnp.maximum(earlier, merged[0])
    for k in (2, 3, 1):
        earlier = jnp.maximum(earlier, send(merged[k], other(k)))
    return earlier, later


def solution(mesh):
    return jax.shard_map(
        shards,
        mesh=mesh,
        in_specs=(P(("blk", "rep"), None), P()),
        out_specs=(P(("blk", "rep")), P(("blk", "rep"))),
        check_vma=False,
    )
```

```python
import jax
import jax.numpy as jnp
from jax import lax
from jax.sharding import PartitionSpec as P


AXES = ("blk", "rep")
LINE = 8
LOW = -1.0


def routes(blocks, move):
    pairs = []
    for block in range(blocks):
        for place in range(4):
            target = move(block, place)
            if target is not None:
                pairs.append((4 * block + place, target[0] % blocks * 4 + target[1]))
    return pairs


def onward(block, place):
    return block + 1, place ^ 2 if block % LINE == LINE - 1 else place


def back(block, place):
    return block - 1, place ^ 2 if block % LINE == 0 else place


def back_twice(block, place):
    return back(*back(block, place))


def other(bits):
    return lambda block, place: (block, place ^ bits)


def scores_of(left, right):
    return lax.dot_general(
        left, right, (((1,), (1,)), ((), ())), preferred_element_type=jnp.float32
    )


def best_pair(host, host_rank, visit, visit_rank):
    kept = jnp.where(
        visit_rank[None, :] < host_rank[:, None], scores_of(host, visit), jnp.float32(LOW)
    )
    return jnp.max(kept, axis=1), jnp.max(kept, axis=0)


def own_pair(own, own_rank, peer, peer_rank):
    earlier = jnp.where(
        peer_rank[None, :] < own_rank[:, None], scores_of(own, peer), jnp.float32(LOW)
    )
    later = jnp.where(
        own_rank[None, :] < peer_rank[:, None], scores_of(peer, own), jnp.float32(LOW)
    )
    return jnp.max(earlier, axis=1), jnp.max(later, axis=0)


def largest(values):
    best = values[0]
    for value in values[1:]:
        best = jnp.maximum(best, value)
    return best


def shards(embeddings, ranks):
    rows = embeddings.shape[0]
    blocks = lax.axis_size("blk")
    block = lax.axis_index("blk")
    place = lax.axis_index("rep")
    z = block % LINE

    def send(value, move):
        return lax.ppermute(value, AXES, routes(blocks, move))

    def ranks_of(block_id, place_id):
        start = (block_id * 4 + place_id) * rows
        return lax.dynamic_slice_in_dim(ranks, start, rows)

    squares = jnp.sum(embeddings * embeddings, axis=1, keepdims=True)
    unit = (embeddings * lax.rsqrt(squares + 1e-06)).astype(jnp.bfloat16)

    def pieces(values, move):
        return [send(value, move) for value in values]

    ups = pieces(jnp.split(unit, [256]), onward)
    downs = pieces(jnp.split(unit, [256]), back)
    across = send(unit, other(2))
    beside = send(unit, other(1))
    upps = pieces(ups, onward)
    downs_across = pieces(downs, other(2))
    across_beside = send(across, other(1))
    visit1 = jnp.concatenate(ups)
    ahead = jnp.concatenate(downs)
    visit2 = jnp.concatenate(upps)
    ahead_across = jnp.concatenate(downs_across)
    ahead_beside = send(ahead, other(1))
    ahead_both = send(ahead_across, other(1))

    host = [unit, beside, across, across_beside]
    host_ranks = [ranks_of(block, place ^ k) for k in range(4)]
    prev = (block + blocks - 1) % blocks
    prev2 = (block + blocks - 2) % blocks
    nxt = (block + 1) % blocks
    prev_place = jnp.where(z == 0, place ^ 2, place)
    prev2_place = jnp.where(z <= 1, place ^ 2, place)
    next_place = jnp.where(z == LINE - 1, place ^ 2, place)
    rank1 = ranks_of(prev, prev_place)
    rank2 = ranks_of(prev2, prev2_place)
    front = [ahead, ahead_beside, ahead_across, ahead_both]
    front_ranks = [ranks_of(nxt, next_place ^ k) for k in range(4)]

    def tiles(pair, left, left_ranks, right, right_rank):
        out = []
        for k in range(4):
            out.append(pair(left[k], left_ranks[k], right, right_rank))
        return out

    own = []
    for k in range(4):
        own.append(own_pair(unit, host_ranks[0], host[k], host_ranks[k]))
    earlier = largest([pair[0] for pair in own])
    later = largest([pair[1] for pair in own])

    one = tiles(best_pair, host, host_ranks, visit1, rank1)
    two = tiles(best_pair, front, front_ranks, visit1, rank1)
    columns1 = largest([pair[1] for pair in one + two])
    three = tiles(best_pair, front, front_ranks, visit2, rank2)
    columns2 = largest([pair[1] for pair in three])
    front_rows = jnp.stack([jnp.maximum(a[0], b[0]) for a, b in zip(two, three)])
    host_rows = jnp.stack([pair[0] for pair in one])

    merged = jnp.maximum(host_rows, send(front_rows, onward))
    later = jnp.maximum(later, send(columns1, back))
    later = jnp.maximum(later, send(columns2, back_twice))
    earlier = jnp.maximum(earlier, merged[0])
    for k in (2, 3, 1):
        earlier = jnp.maximum(earlier, send(merged[k], other(k)))
    return earlier, later


def solution(mesh):
    return jax.shard_map(
        shards,
        mesh=mesh,
        in_specs=(P(("blk", "rep"), None), P()),
        out_specs=(P(("blk", "rep")), P(("blk", "rep"))),
        check_vma=False,
    )
```

```python
import jax
import jax.numpy as jnp
from jax import lax
from jax.sharding import PartitionSpec as P


AXES = ("blk", "rep")
LINE = 8
LOW = -1.0


def routes(blocks, move):
    pairs = []
    for block in range(blocks):
        for place in range(4):
            target = move(block, place)
            if target is not None:
                pairs.append((4 * block + place, target[0] % blocks * 4 + target[1]))
    return pairs


def onward(block, place):
    return block + 1, place ^ 2 if block % LINE == LINE - 1 else place


def back(block, place):
    return block - 1, place ^ 2 if block % LINE == 0 else place


def back_twice(block, place):
    return back(*back(block, place))


def other(bits):
    return lambda block, place: (block, place ^ bits)


def scores_of(left, right):
    return lax.dot_general(
        left, right, (((1,), (1,)), ((), ())), preferred_element_type=jnp.float32
    )


def best_pair(host, host_rank, visit, visit_rank):
    kept = jnp.where(
        visit_rank[None, :] < host_rank[:, None], scores_of(host, visit), jnp.float32(LOW)
    )
    return jnp.max(kept, axis=1), jnp.max(kept, axis=0)


def largest(values):
    best = values[0]
    for value in values[1:]:
        best = jnp.maximum(best, value)
    return best


def shards(embeddings, ranks):
    rows = embeddings.shape[0]
    blocks = lax.axis_size("blk")
    block = lax.axis_index("blk")
    place = lax.axis_index("rep")
    z = block % LINE

    def send(value, move):
        return lax.ppermute(value, AXES, routes(blocks, move))

    def ranks_of(block_id, place_id):
        start = (block_id * 4 + place_id) * rows
        return lax.dynamic_slice_in_dim(ranks, start, rows)

    def normalised(values):
        squares = jnp.sum(values * values, axis=1, keepdims=True)
        return (values * lax.rsqrt(squares + 1e-06)).astype(jnp.bfloat16)

    halves = [normalised(half) for half in jnp.split(embeddings, 2)]
    unit = jnp.concatenate(halves)

    def pieces(values, move):
        return [send(value, move) for value in values]

    ups = pieces(halves, onward)
    downs = pieces(halves, back)
    across = send(unit, other(2))
    beside = send(unit, other(1))
    upps = pieces(ups, onward)
    downs_across = pieces(downs, other(2))
    across_beside = send(across, other(1))
    visit1 = jnp.concatenate(ups)
    ahead = jnp.concatenate(downs)
    visit2 = jnp.concatenate(upps)
    ahead_across = jnp.concatenate(downs_across)
    ahead_beside = send(ahead, other(1))
    ahead_both = send(ahead_across, other(1))

    host = [unit, beside, across, across_beside]
    host_ranks = [ranks_of(block, place ^ k) for k in range(4)]
    prev = (block + blocks - 1) % blocks
    prev2 = (block + blocks - 2) % blocks
    nxt = (block + 1) % blocks
    prev_place = jnp.where(z == 0, place ^ 2, place)
    prev2_place = jnp.where(z <= 1, place ^ 2, place)
    next_place = jnp.where(z == LINE - 1, place ^ 2, place)
    rank1 = ranks_of(prev, prev_place)
    rank2 = ranks_of(prev2, prev2_place)
    front = [ahead, ahead_beside, ahead_across, ahead_both]
    front_ranks = [ranks_of(nxt, next_place ^ k) for k in range(4)]

    def tiles(pair, left, left_ranks, right, right_rank):
        out = []
        for k in range(4):
            out.append(pair(left[k], left_ranks[k], right, right_rank))
        return out

    own = tiles(best_pair, host, host_ranks, unit, host_ranks[0])
    one = tiles(best_pair, host, host_ranks, visit1, rank1)
    two = tiles(best_pair, front, front_ranks, visit1, rank1)
    columns1 = largest([pair[1] for pair in one + two])
    three = tiles(best_pair, front, front_ranks, visit2, rank2)
    columns2 = largest([pair[1] for pair in three])
    front_rows = jnp.stack([jnp.maximum(a[0], b[0]) for a, b in zip(two, three)])
    host_rows = jnp.stack([jnp.maximum(a[0], b[0]) for a, b in zip(own, one)])

    merged = jnp.maximum(host_rows, send(front_rows, onward))
    later = largest([pair[1] for pair in own])
    later = jnp.maximum(later, send(columns1, back))
    later = jnp.maximum(later, send(columns2, back_twice))
    earlier = merged[0]
    for k in (2, 3, 1):
        earlier = jnp.maximum(earlier, send(merged[k], other(k)))
    return earlier, later


def solution(mesh):
    return jax.shard_map(
        shards,
        mesh=mesh,
        in_specs=(P(("blk", "rep"), None), P()),
        out_specs=(P(("blk", "rep")), P(("blk", "rep"))),
        check_vma=False,
    )
```
